32 devices in a mesh: row: 8 (over z, x), col: 2 (over y), depth: 2 (over core).
Axes of the slice: x: 2, y: 2, z: 4, core: 2. Of those that a mesh axis runs over, the one named last changes fastest.
Arguments:
- tokens: bfloat16 [1024, 5376], P('row', 'depth'), may hold values from -6 to 6
- gate_weight: bfloat16 [9216, 5376], P(('col', 'row'), 'depth'), may hold values from -0.078125 to 0.078125
- up_weight: bfloat16 [9216, 5376], P(('col', 'row'), 'depth'), may hold values from -0.078125 to 0.078125
- down_weight: bfloat16 [9216, 5376], P(('col', 'depth'), 'row'), may hold values from -0.09375 to 0.09375
Outputs:
- output: bfloat16 [1024, 5376], P('row', ('col', 'depth'))
The draws below stay inside these ranges and needn't reach their ends.
All inputs are finite; a program needn't handle non-finite values.
Results may differ from the reference program's by a relative error of at most 0.0049.
Values may be sent and summed in bfloat16 or wider, within the bound.
A program may use at most 128 MiB of HBM per device.

```python
import jax
import jax.numpy as jnp

D = 5376
FFW = 9216
TOKENS = 1024


def strengthened(result, key, source, target, parts, factor):
    def block_of(dim):
        return (jnp.arange(result.shape[dim]) // (result.shape[dim] // parts)).reshape((-1,) + (1,) * (result.ndim - 1 - dim))

    one_side = jax.random.permutation(key, parts)[block_of(target)]
    second = (block_of(target) + parts // 2) % parts
    return jnp.where((block_of(source) == one_side) | (block_of(source) == second), factor * result, result)


def level_of(own_key, extent, split, smallest, largest):
    factor_of, own = 1.0, jax.random.fold_in(own_key, 6)
    for axis_at, blocks in split:
        draws = jnp.exp(jax.random.uniform(jax.random.fold_in(own, axis_at), (blocks,), jnp.float32, smallest / len(split), largest / len(split)))
        factor_of = factor_of * jnp.repeat(draws, extent[axis_at] // blocks).reshape([-1 if axis == axis_at else 1 for axis in range(len(extent))])
    return factor_of


def gaussian(rng, dims, spread, limit, pieces=(), held_as=jnp.bfloat16):
    loudness = level_of(rng, dims, pieces, -0.22, 0.18) if pieces else 1.0
    result = jax.random.normal(rng, dims, jnp.float32) * spread * loudness
    return jnp.minimum(jnp.maximum(result, -limit), limit).astype(held_as)


def noise_with(key, dims, spread, most, shards, heavy, dtype=jnp.bfloat16):
    result = spread * jax.random.normal(key, dims, jnp.float32)
    if shards:
        result = result * level_of(key, dims, shards, -0.22, 0.18)
    return jnp.clip(strengthened(result, jax.random.fold_in(key, 3), *heavy), -most, most).astype(dtype)


def setup_inputs(seed: int = 0) -> dict:
    key_of = jax.random.split(jax.random.key(seed), 5)
    tokens = gaussian(key_of[0], (TOKENS, D), 1.0, 6.0, ((0, 8), (1, 2)))
    gate_weight = gaussian(key_of[1], (FFW, D), D ** -0.5, 0.078125, ((0, 16), (1, 2)))
    up_weight = gaussian(key_of[2], (FFW, D), D ** -0.5, 0.078125, ((0, 16), (1, 2)))
    down_weight = noise_with(key_of[3], (FFW, D), FFW ** -0.5, 0.09375, ((0, 4), (1, 8)), (0, 1, 8, 2.0))
    return dict(tokens=tokens, gate_weight=gate_weight, up_weight=up_weight, down_weight=down_weight)


def reference(tokens, gate_weight, up_weight, down_weight):
    gate_part = jnp.dot(tokens, gate_weight.T, preferred_element_type=jnp.float32)
    up_part = jnp.dot(tokens, up_weight.T, preferred_element_type=jnp.float32)
    hidden = (jax.nn.silu(gate_part) * up_part).astype(jnp.bfloat16)
    return jnp.dot(hidden, down_weight, preferred_element_type=jnp.float32).astype(jnp.bfloat16)
```

```python
import functools

import jax
import jax.numpy as jnp
from jax import lax
from jax.experimental import pallas as pl
from jax.experimental.pallas import tpu as pltpu
from jax.sharding import PartitionSpec as P

MESH = pl.DeviceIdType.MESH
F32 = jnp.float32
BF16 = jnp.bfloat16


def row_at(place, n):
    back = place // (n // 2)
    return 2 * place * (1 - back) + (2 * (n - 1 - place) + 1) * back


UNITS, SPLIT = 4, 2
RING = (3, 2, 2, 2)
PLAN = [
    ("G", 0), ("T", 1, 0), ("H", 0, 1, 0), ("T", 1, 1), ("T", 2, 0), ("T", 1, 2), ("T", 2, 1), ("G", 1),
    ("H", 0, 2, 0), ("T", 3, 0), ("T", 3, 1), ("H", 1, 1, 0), ("G", 2), ("T", 4, 0), ("H", 1, 1, 1), ("A", 1, 1),
    ("H", 1, 2, 0), ("H", 2, 1, 0), ("T", 4, 1), ("H", 0, 3, 0), ("H", 1, 2, 1), ("H", 1, 3, 0), ("A", 0, 3),
    ("H", 2, 2, 0), ("H", 2, 1, 1), ("G", 3), ("H", 0, 4, 0), ("H", 1, 3, 1), ("H", 2, 3, 0), ("A", 0, 4),
    ("H", 1, 4, 0), ("A", 1, 0), ("A", 2, 1), ("H", 2, 2, 1), ("A", 2, 2), ("A", 1, 3), ("H", 3, 1, 0), ("G", 4),
    ("A", 4, 0), ("H", 3, 1, 1), ("A", 3, 1), ("H", 1, 4, 1), ("F1", 4), ("A", 0, 2), ("H", 3, 2, 0), ("A", 3, 0),
    ("A", 2, 0), ("F2", 4), ("H", 4, 1, 0), ("A", 1, 4), ("A", 4, 1), ("A", 1, 2), ("H", 3, 2, 1), ("H", 2, 3, 1),
    ("A", 0, 1), ("A", 3, 2), ("A", 0, 0), ("H", 3, 3, 0), ("A", 2, 3), ("F1", 3), ("H", 4, 2, 0), ("F2", 3),
    ("A", 4, 2), ("H", 3, 3, 1), ("F3", 4), ("H", 2, 4, 0), ("A", 3, 3), ("H", 2, 4, 1), ("A", 2, 4), ("F1", 2),
    ("H", 3, 4, 0), ("H", 4, 3, 0), ("F2", 2), ("A", 4, 3), ("H", 3, 4, 1), ("F3", 3), ("A", 3, 4), ("F1", 1),
    ("F2", 1), ("H", 4, 4, 0), ("A", 4, 4), ("F1", 0), ("F3", 2), ("F2", 0), ("F3", 1), ("F3", 0),
]


def kernel(n, counts, tok_hbm, gate_hbm, up_hbm, down_hbm, out_ref, tok, weights, down, part, keep, theirs, hid, total, other,
           own_half, send_y, from_y, done, land, other0, half0, send0, land0, load_sem, down_send, down_recv,
           tok_send, tok_recv, y_send, y_recv, part_send, part_recv, hid_send, hid_recv, sum_send, sum_recv,
           col_send, col_recv, out_send, out_recv, last_send, last_recv):
    row, col, core = lax.axis_index("row"), lax.axis_index("col"), lax.axis_index("depth")
    half = n // 2
    x, z = row % 2, row // 2
    place = z * (1 - x) + (n - 1 - z) * x
    ways = ({"row": row_at((place + 1) % n, n)}, {"row": row_at((place + n - 1) % n, n)})
    beside, partner = {"col": 1 - col}, {"depth": 1 - core}
    block = tok_hbm.shape[0]
    units = gate_hbm.shape[0]
    share = units // 2
    features, held = down_hbm.shape
    middle = features // 2
    window = hid.shape[2]
    unit_rows = block // UNITS

    def remote(src, dst, send, recv, to):
        return pltpu.make_async_remote_copy(src_ref=src, dst_ref=dst, send_sem=send, recv_sem=recv,
                                            device_id=to, device_id_type=MESH)

    loads = [pltpu.make_async_copy(tok_hbm, tok.at[0], load_sem.at[0]),
             pltpu.make_async_copy(gate_hbm, weights.at[0], load_sem.at[1]),
             pltpu.make_async_copy(up_hbm, weights.at[1], load_sem.at[2]),
             pltpu.make_async_copy(down_hbm, down.at[:, pl.ds(0, held)], load_sem.at[3])]
    for copy in loads:
        copy.start()
    barrier = pltpu.get_barrier_semaphore()
    for peer in ways + (beside, partner):
        pl.semaphore_signal(barrier, inc=1, device_id=peer, device_id_type=MESH)
    with jax.named_scope("barrier"):
        pl.semaphore_wait(barrier, 4)
    with jax.named_scope("tokload"):
        loads[0].wait()

    def slot(hop, way):
        return 0 if hop == 0 else 1 if hop == half else 2 * hop + way

    def rounds(hop, unit):
        return (2 * unit // RING[hop - 1],) if hop == half else (0, 1)

    tok_keys, y_keys, hid_keys, whole = {}, {}, {}, []

    def number(keys, *key):
        return keys.setdefault(key, len(keys))

    def unit_at(unit, side):
        return pl.ds(pl.multiple_of(unit_rows * (unit * (1 - side) + (UNITS - 1 - unit) * side), unit_rows), unit_rows)

    def tok_copy(hop, way, unit):
        rows = unit_at(unit, col)
        return remote(tok.at[slot(hop - 1, way), rows], tok.at[slot(hop, way), rows],
                      tok_send, tok_recv.at[number(tok_keys, way, hop, unit)], ways[way])

    def y_copy(at, unit, side):
        rows = unit_at(unit, side)
        return remote(tok.at[at, rows], tok.at[at, rows], y_send, y_recv.at[number(y_keys, at, unit)], beside)

    for unit in range(RING[0]):
        for way in (0, 1):
            tok_copy(1, way, unit).start()

    def row_shift(source):
        return pl.multiple_of(source // half * 2 * (share % 128) + core * (share % 128), share % 128)

    given = down.at[:, pl.ds(held, half * window)]
    give = []
    for i in range(half):
        q = 2 * i + 1 - core
        lanes = pl.ds(pl.multiple_of(q * share // 128 * 128, 128), window)
        give.append(remote(down.at[:, lanes], down.at[:, pl.ds(held + i * window, window)],
                           down_send, down_recv, partner))

    def product(kind, which, slots):
        rows = pl.ds(pl.multiple_of(which * share, 16), share)
        seen = tok[slots[0]:slots[0] + len(slots)].reshape(block * len(slots), tok.shape[2])
        return lax.dot_general(weights[kind, rows, :], seen, (((1,), (1,)), ((), ())), preferred_element_type=F32)

    def lanes_of(piece):
        return (half - 1, 0, block) if piece == 0 else (half - 1, block, block) if piece == half else (
            piece - 1, 0, 2 * block)

    def parts_of(piece):
        return 1 if piece in (0, half) else SPLIT

    def hid_at(at, piece, source, part_of):
        index, first, wide = lanes_of(piece)
        wide = wide // parts_of(piece)
        return hid.at[at, index, pl.ds(row_shift(source), share), pl.ds(first + part_of * wide, wide)]

    def hid_sems(piece, hop, way, part_of):
        return hid_send, hid_recv.at[number(hid_keys, way, hop, piece, part_of)], ways[way]

    def hid_copy(piece, hop, way, part_of):
        source = (place + (n - hop + 1 if way == 0 else hop - 1)) % n
        return remote(hid_at(slot(hop - 1, way), piece, source, part_of), hid_at(slot(hop, way), piece, source, part_of),
                      *hid_sems(piece, hop, way, part_of))

    def hid_wait(piece, hop, way, part_of):
        source = (place + (n - hop if way == 0 else hop)) % n
        at = hid_at(slot(hop, way), piece, source, part_of)
        remote(at, at, *hid_sems(piece, hop, way, part_of)).wait_recv()

    def hid_rounds(piece, hop):
        return (piece % 2,) if hop == half else (0, 1)

    def swap(group, kind, wide):
        return remote(part.at[group, kind, :, pl.ds(0, wide)], theirs.at[group, kind, :, pl.ds(0, wide)],
                      part_send, part_recv.at[group], partner)

    def gate_up(group):
        slots = [0] if group == 0 else [1] if group == half else [2 * group, 2 * group + 1]
        wide = block * len(slots)
        if group == 0:
            loads[1].wait()
            loads[2].wait()
        else:
            for unit in range(UNITS - RING[group - 1]):
                for way in rounds(group, unit):
                    with jax.named_scope(f"ywait#g={group}#u={unit}#w={way}"):
                        y_copy(slot(group, way), unit, 1 - col).wait_recv()
        for kind in (0, 1):
            part[group, kind, :, :wide] = product(kind, 1 - core, slots)
            swap(group, kind, wide).start()
        for kind in (0, 1):
            keep[kind, :, :wide] = product(kind, core, slots)
        if group == 0:
            loads[3].wait()
            for copy in give:
                copy.start()
        with jax.named_scope(f"swapwait#g={group}"):
            both = theirs.at[group, :, :, pl.ds(0, wide)]
            remote(both, both, part_send, part_recv.at[group], partner).wait_recv()
        gate = keep[0, :, :wide] + theirs[group, 0, :, :wide]
        up = keep[1, :, :wide] + theirs[group, 1, :, :wide]
        index, first, wide = lanes_of(group)
        hid[0, index, pl.ds(row_shift(place), share), first:first + wide] = (
            gate / (1.0 + jnp.exp(-gate)) * up).astype(BF16)
        for part_of in range(parts_of(group)):
            for way in (0, 1):
                hid_copy(group, 1, way, part_of).start()

    def token_hop(hop, unit):
        for way in rounds(hop, unit):
            with jax.named_scope(f"tokwait#h={hop}#u={unit}#w={way}"):
                tok_copy(hop, way, unit).wait_recv()
            if hop < half and unit < RING[hop] and way in rounds(hop + 1, unit):
                tok_copy(hop + 1, way, unit).start()
            if unit < UNITS - RING[hop - 1]:
                y_copy(slot(hop, way), unit, col).start()

    def hid_hop(piece, hop, part_of):
        for way in hid_rounds(piece, hop):
            with jax.named_scope(f"hidwait#p={piece}#h={hop}#q={part_of}#w={way}"):
                hid_wait(piece, hop, way, part_of)
            if hop < half and way in hid_rounds(piece, hop + 1):
                hid_copy(piece, hop + 1, way, part_of).start()

    def add_one(at, source, piece):
        index, first, wide = lanes_of(piece)
        at_row = row_at(source, n)
        same = 1 - (at_row // half - core) * (at_row // half - core)
        mine = (2 * (at_row % half) + core) * share // 128 * 128
        start = pl.multiple_of(same * mine + (1 - same) * (held + at_row % half * window), 128)
        term = lax.dot_general(down[:, pl.ds(start, window)], hid[at, index, :, first:first + wide],
                               (((1,), (0,)), ((), ())), preferred_element_type=F32)
        if piece in (0, half):
            total[(source + piece) % n] += term
        else:
            for k, token_block in enumerate(((source + n - piece) % n, (source + piece) % n)):
                total[token_block] += term[:, k * block:(k + 1) * block]

    def add_down(piece, hop):
        if not whole:
            whole.append(True)
            remote(given, given, down_send, down_recv, partner).wait_recv()
        if hop == 0:
            add_one(0, place, piece)
        elif hop == half:
            add_one(1, (place + half) % n, piece)
        else:
            @pl.loop(0, 2)
            def _(way):
                add_one(2 * hop + way, (place + n - hop + 2 * hop * way) % n, piece)

    to_col, to_core = z // 2, z % 2
    near_col = 1 - (col - to_col) * (col - to_col)
    near_core = 1 - (core - to_core) * (core - to_core)

    def handled(d, by):
        return (place + half) % n if d == half else (place + d + (n - 2 * d) * by) % n

    def keep_rows(which):
        return pl.ds(pl.multiple_of(which * middle, 16), middle)

    def sum_copy(d):
        return remote(total.at[handled(d, 1 - core)], other.at[d - 1], sum_send.at[d - 1], sum_recv.at[d - 1], partner)

    def col_copy(d):
        return remote(send_y.at[d - 1], from_y.at[d - 1], col_send.at[d - 1], col_recv.at[d - 1], beside)

    def out_copy(d):
        to = {"row": row_at(handled(d, core), n), "col": to_col, "depth": to_core}
        return remote(done.at[d - 1], land.at[x, col], out_send.at[d - 1], out_recv.at[x, col], to)

    def near_copy():
        return remote(total.at[place], other0, last_send.at[0], last_recv.at[0], partner)

    def half_copy():
        return remote(total.at[place, keep_rows(1 - core)], half0, last_send.at[1], last_recv.at[1], partner)

    def far_copy():
        return remote(send0, land0.at[core], last_send.at[2], last_recv.at[2 + core], {"col": to_col, "depth": to_core})

    def only(d, who):
        return pl.when(core == who) if d == half else (lambda f: f())

    def final_1(d):
        if d:
            @only(d, 1)
            def _():
                sum_copy(d).start()
            return

        @pl.when(near_col * (1 - near_core) == 1)
        def _():
            near_copy().start()

        @pl.when(near_col == 0)
        def _():
            half_copy().start()

    def final_2(d):
        if d:
            @only(d, 0)
            def _():
                with jax.named_scope(f"sumwait#d={d}"):
                    sum_copy(d).wait_recv()
                at = handled(d, core)
                send_y[d - 1] = (total[at, keep_rows(1 - col)] + other[d - 1, keep_rows(1 - col)]).astype(BF16)
                col_copy(d).start()
                own_half[d - 1] = total[at, keep_rows(col)] + other[d - 1, keep_rows(col)]
            return

        @pl.when(near_col == 0)
        def _():
            half_copy().wait_recv()
            send0[...] = (total[place, keep_rows(core)] + half0[...]).astype(BF16)
            far_copy().start()

    def final_3(d):
        if d:
            @only(d, 0)
            def _():
                with jax.named_scope(f"colwait#d={d}"):
                    col_copy(d).wait_recv()
                done[d - 1] = (own_half[d - 1] + from_y[d - 1].astype(F32)).astype(BF16)
                out_copy(d).start()
            return

        @pl.when(near_col * near_core == 1)
        def _():
            with jax.named_scope("lastwait"):
                near_copy().wait_recv()
                for which in (0, 1):
                    remote(send0, land0.at[which], last_send.at[2], last_recv.at[2 + which], beside).wait_recv()
            for which in (0, 1):
                rows = slice(which * middle, (which + 1) * middle)
                value = total[place, rows] + other0[rows] + land0[which].astype(F32)
                out_ref[pl.ds(pl.multiple_of(x * features + which * middle, 16), middle)] = value.astype(BF16)

    total[...] = jnp.zeros_like(total)
    gap = window - share
    for at in range(n):
        hop, way = (0, 0) if at == 0 else (half, 0) if at == 1 else (at // 2, at % 2)
        shift = row_shift((place + (n - hop if way == 0 else hop)) % n)
        unit = share % 128
        for k in range(gap // unit):
            below = jnp.where(k * unit < shift, 0, share)
            rows = pl.ds(pl.multiple_of(k * unit + below, unit), unit)
            for index in range(half):
                hid[at, index, rows, :] = jnp.zeros((unit, 2 * block), BF16)

    act = {"G": gate_up, "T": token_hop, "H": hid_hop, "A": add_down, "F1": final_1, "F2": final_2, "F3": final_3}
    for name, *args in PLAN:
        with jax.named_scope(name + "_" + "_".join(map(str, args))):
            act[name](*args)

    with jax.named_scope("outwait"):
        for xx in (0, 1):
            self = near_col * near_core * (1 - (x - xx) * (x - xx))

            @pl.when(self == 0)
            def _():
                for yy in (0, 1):
                    remote(land.at[xx, yy], land.at[xx, yy], out_send.at[0], out_recv.at[xx, yy], beside).wait_recv()
                    first = xx * features + yy * middle
                    out_ref[first:first + middle] = land[xx, yy]
    with jax.named_scope("sendwait"):
        for d in range(1, half + 1):
            @only(d, 1)
            def _():
                sum_copy(d).wait_send()

            @only(d, 0)
            def _():
                col_copy(d).wait_send()
                out_copy(d).wait_send()

        @pl.when(near_col * (1 - near_core) == 1)
        def _():
            near_copy().wait_send()

        @pl.when(near_col == 0)
        def _():
            half_copy().wait_send()
            far_copy().wait_send()
        tok_sent, y_sent = tok.at[0:counts[0] // UNITS], tok.at[0:counts[1] // UNITS]
        hid_sent, part_sent = hid.at[0:n - 1, :, pl.ds(0, share)], part.at[0:half]
        for sent, sem in ((tok_sent, tok_send), (y_sent, y_send), (hid_sent, hid_send), (part_sent, part_send),
                          (given, down_send)):
            remote(sent, sent, sem, last_recv.at[0], partner).wait_send()


def fused_block(n, tokens, gate_weight, up_weight, down_weight):
    block, width = tokens.shape
    units = gate_weight.shape[0]
    held, features = down_weight.shape
    half, share = n // 2, units // 2
    window = (share + 127) // 128 * 128
    middle = features // 2
    counts = (2 * sum(RING[:-1]) + RING[-1], (n - 1) * UNITS - 2 * sum(RING[:-1]) - RING[-1],
              (n - 1) * (2 + SPLIT * (half - 1)))
    dma = pltpu.SemaphoreType.DMA
    result = pl.pallas_call(
        functools.partial(kernel, n, counts),
        out_shape=jax.ShapeDtypeStruct((2 * features, block), BF16),
        in_specs=[pl.BlockSpec(memory_space=pltpu.HBM)] * 4,
        out_specs=pl.BlockSpec(memory_space=pltpu.VMEM),
        scratch_shapes=[
            pltpu.VMEM((n, block, width), BF16),
            pltpu.VMEM((2, units, width), BF16),
            pltpu.VMEM((features, held + half * window), BF16),
            pltpu.VMEM((half + 1, 2, share, 2 * block), F32),
            pltpu.VMEM((2, share, 2 * block), F32),
            pltpu.VMEM((half + 1, 2, share, 2 * block), F32),
            pltpu.VMEM((n, half, window, 2 * block), BF16),
            pltpu.VMEM((n, features, block), F32),
            pltpu.VMEM((half, features, block), F32),
            pltpu.VMEM((half, middle, block), F32),
            pltpu.VMEM((half, middle, block), BF16),
            pltpu.VMEM((half, middle, block), BF16),
            pltpu.VMEM((half, middle, block), BF16),
            pltpu.VMEM((2, 2, middle, block), BF16),
            pltpu.VMEM((features, block), F32),
            pltpu.VMEM((middle, block), F32),
            pltpu.VMEM((middle, block), BF16),
            pltpu.VMEM((2, middle, block), BF16),
            dma((4,)), dma(()), dma(()),
            dma(()), dma((counts[0],)),
            dma(()), dma((counts[1],)),
            dma(()), dma((half + 1,)),
            dma(()), dma((counts[2],)),
            dma((half,)), dma((half,)),
            dma((half,)), dma((half,)),
            dma((half,)), dma((2, 2)),
            dma((3,)), dma((4,)),
        ],
        compiler_params=pltpu.CompilerParams(
            collective_id=0, has_side_effects=True, vmem_limit_bytes=54528 * 1024
        ),
    )(tokens, gate_weight, up_weight, down_weight.T)
    return result.T


def send_out(mine, rows, cols, depths):
    quarters = cols * depths
    per = rows // quarters
    block = mine.shape[0] // per
    width = mine.shape[1]
    row = lax.axis_index("row")
    low = row % per
    got = jnp.zeros((block, per, width), jnp.bfloat16)
    for k in range(per):
        pairs = []
        for r in range(rows):
            for q in range(quarters):
                a, e = r // per, r % per
                to_row = q * per + (e + k) % per
                pairs.append((r * quarters + q, to_row * quarters + a))
        piece = lax.dynamic_slice_in_dim(mine, (low + k) % per * block, block, 0)
        piece = lax.ppermute(piece, ("row", "col", "depth"), pairs)
        got = lax.dynamic_update_slice_in_dim(got, piece[:, None], (low - k) % per, 1)
    return got.reshape(block, per * width)


def solution(mesh):
    rows, cols, depths = (mesh.shape[a] for a in ("row", "col", "depth"))

    def local(tokens, gate_weight, up_weight, down_weight):
        units = gate_weight.shape[0]
        every = lax.all_gather(tokens, "row", axis=0, tiled=True)
        down = down_weight.reshape(rows // depths, depths, units // depths, -1)
        down = lax.all_to_all(down, "depth", split_axis=1, concat_axis=0, tiled=True)
        down = down.reshape(rows, units // depths, -1)
        paired = jnp.stack([gate_weight, up_weight])
        sums = jnp.einsum("td,gfd->gtf", every, paired, preferred_element_type=jnp.float32)
        sums = lax.psum_scatter(sums, "depth", scatter_dimension=2, tiled=True)
        hidden = (jax.nn.silu(sums[0]) * sums[1]).astype(jnp.bfloat16)
        hidden = lax.all_gather(hidden, "row", axis=0)
        partial = jnp.einsum("rtk,rkc->tc", hidden, down, preferred_element_type=jnp.float32)
        mine = lax.psum_scatter(partial, ("col", "depth"), scatter_dimension=0, tiled=True)
        return send_out(mine.astype(BF16), rows, cols, depths)

    def fused(*args):
        return fused_block(rows, *args)

    in_specs = (
        P("row", "depth"),
        P(("col", "row"), "depth"),
        P(("col", "row"), "depth"),
        P(("col", "depth"), "row"),
    )
    out_specs = P("row", ("col", "depth"))
    small = cols == 2 and depths == 2 and rows == 8
    return jax.shard_map(fused if small else local, mesh=mesh, in_specs=in_specs, out_specs=out_specs, check_vma=False)
```

```python
import functools

import jax
import jax.numpy as jnp
from jax import lax
from jax.experimental import pallas as pl
from jax.experimental.pallas import tpu as pltpu
from jax.sharding import PartitionSpec as P

MESH = pl.DeviceIdType.MESH
F32 = jnp.float32
BF16 = jnp.bfloat16


def row_at(place, n):
    back = place // (n // 2)
    return 2 * place * (1 - back) + (2 * (n - 1 - place) + 1) * back


UNITS = 8
SPLIT = (1, 2, 2, 2, 2)
RING = (5, 4, 4, 4)
PLAN = [
    ("G", 0), ("T", 1, 0), ("T", 1, 1), ("T", 1, 2), ("T", 2, 0), ("T", 1, 3), ("T", 2, 1), ("T", 2, 2),
    ("T", 1, 4), ("G", 1), ("H", 0, 1, 0), ("T", 2, 3), ("T", 3, 0), ("T", 3, 1), ("H", 1, 1, 0), ("H", 0, 2, 0),
    ("T", 3, 2), ("T", 3, 3), ("H", 1, 1, 1), ("G", 2), ("H", 1, 2, 1), ("H", 2, 1, 0), ("H", 2, 1, 1),
    ("H", 1, 2, 0), ("T", 4, 0), ("A", 2, 0), ("A", 2, 1), ("A", 0, 1), ("T", 4, 1), ("H", 2, 2, 0), ("T", 4, 2),
    ("H", 1, 3, 1), ("T", 4, 3), ("H", 0, 3, 0), ("G", 3), ("H", 1, 3, 0), ("H", 2, 2, 1), ("A", 1, 2),
    ("H", 2, 3, 0), ("A", 2, 2), ("A", 0, 2), ("A", 0, 3), ("A", 0, 0), ("A", 1, 3), ("A", 3, 0), ("H", 3, 1, 0),
    ("G", 4), ("A", 4, 0), ("H", 3, 1, 1), ("H", 0, 4, 0), ("A", 0, 4), ("A", 3, 1), ("F1", 4), ("H", 1, 4, 0),
    ("A", 1, 1), ("H", 1, 4, 1), ("H", 3, 2, 0), ("H", 4, 1, 0), ("F2", 4), ("A", 1, 4), ("A", 1, 0),
    ("H", 4, 1, 1), ("A", 4, 1), ("H", 3, 2, 1), ("H", 2, 3, 1), ("A", 2, 3), ("H", 2, 4, 0), ("A", 3, 2),
    ("F1", 3), ("H", 3, 3, 0), ("F2", 3), ("H", 4, 2, 0), ("H", 4, 2, 1), ("A", 4, 2), ("H", 3, 3, 1), ("F3", 4),
    ("A", 3, 3), ("H", 2, 4, 1), ("A", 2, 4), ("F1", 2), ("F3", 3), ("H", 4, 3, 0), ("H", 4, 3, 1), ("A", 4, 3),
    ("F2", 2), ("H", 3, 4, 1), ("H", 3, 4, 0), ("A", 3, 4), ("F1", 1), ("F2", 1), ("H", 4, 4, 0), ("H", 4, 4, 1),
    ("A", 4, 4), ("F3", 2), ("F1", 0), ("F2", 0), ("F3", 0),
]


def box_of(rows, n, block, width):
    total = rows * width
    for k in range(n, 0, -1):
        for r in range(block, 0, -16):
            wide = total // (k * r)
            if k * r * wide == total and wide % 128 == 0 and wide <= width:
                return slice(0, k), pl.ds(0, r), pl.ds(0, wide)


def kernel(n, counts, tok_hbm, gate_hbm, up_hbm, down_hbm, out_ref, tok, weights, down, part, keep, theirs, hid, total, other,
           own_half, send_y, from_y, done, land, direct, land1, other0, half0, send0, land0, load_sem, down_send, down_recv,
           tok_send, tok_recv, y_send, y_recv, part_send, part_recv, hid_send, hid_recv, sum_send, sum_recv,
           col_send, col_recv, out_send, out_recv, last_send, last_recv, direct_recv):
    row, col, core = lax.axis_index("row"), lax.axis_index("col"), lax.axis_index("depth")
    half = n // 2
    x, z = row % 2, row // 2
    place = z * (1 - x) + (n - 1 - z) * x
    ways = ({"row": row_at((place + 1) % n, n)}, {"row": row_at((place + n - 1) % n, n)})
    beside, partner = {"col": 1 - col}, {"depth": 1 - core}
    block = tok_hbm.shape[0]
    units = gate_hbm.shape[0]
    share = units // 2
    features, held = down_hbm.shape
    middle = features // 2
    window = hid.shape[2]
    unit_rows = block // UNITS

    def remote(src, dst, send, recv, to):
        return pltpu.make_async_remote_copy(src_ref=src, dst_ref=dst, send_sem=send, recv_sem=recv,
                                            device_id=to, device_id_type=MESH)

    loads = [pltpu.make_async_copy(tok_hbm, tok.at[0], load_sem.at[0]),
             pltpu.make_async_copy(gate_hbm, weights.at[0], load_sem.at[1]),
             pltpu.make_async_copy(up_hbm, weights.at[1], load_sem.at[2]),
             pltpu.make_async_copy(down_hbm, down.at[:, pl.ds(0, held)], load_sem.at[3])]
    for copy in loads:
        copy.start()
    barrier = pltpu.get_barrier_semaphore()
    for peer in ways + (beside, partner):
        pl.semaphore_signal(barrier, inc=1, device_id=peer, device_id_type=MESH)
    with jax.named_scope("barrier"):
        pl.semaphore_wait(barrier, 4)
    with jax.named_scope("tokload"):
        loads[0].wait()

    def slot(hop, way):
        return 0 if hop == 0 else 1 if hop == half else 2 * hop + way

    def rounds(hop, unit):
        return (2 * unit // RING[hop - 1],) if hop == half else (0, 1)

    tok_keys, y_keys, hid_keys, whole = {}, {}, {}, []

    def number(keys, *key):
        return keys.setdefault(key, len(keys))

    def unit_at(unit, side):
        return pl.ds(pl.multiple_of(unit_rows * (unit * (1 - side) + (UNITS - 1 - unit) * side), unit_rows), unit_rows)

    def tok_copy(hop, way, unit):
        rows = unit_at(unit, col)
        return remote(tok.at[slot(hop - 1, way), rows], tok.at[slot(hop, way), rows],
                      tok_send, tok_recv.at[number(tok_keys, way, hop, unit)], ways[way])

    def y_copy(at, unit, side):
        rows = unit_at(unit, side)
        return remote(tok.at[at, rows], tok.at[at, rows], y_send, y_recv.at[number(y_keys, at, unit)], beside)

    for unit in range(RING[0]):
        for way in (0, 1):
            tok_copy(1, way, unit).start()

    def row_shift(source):
        return pl.multiple_of(source // half * 2 * (share % 128) + core * (share % 128), share % 128)

    given = down.at[:, pl.ds(held, half * window)]
    give = []
    for i in range(half):
        q = 2 * i + 1 - core
        lanes = pl.ds(pl.multiple_of(q * share // 128 * 128, 128), window)
        give.append(remote(down.at[:, lanes], down.at[:, pl.ds(held + i * window, window)],
                           down_send, down_recv, partner))

    def product(kind, which, slots):
        rows = pl.ds(pl.multiple_of(which * share, 16), share)
        seen = tok[slots[0]:slots[0] + len(slots)].reshape(block * len(slots), tok.shape[2])
        return lax.dot_general(weights[kind, rows, :], seen, (((1,), (1,)), ((), ())), preferred_element_type=F32)

    def lanes_of(piece):
        return (half - 1, 0, block) if piece == 0 else (half - 1, block, block) if piece == half else (
            piece - 1, 0, 2 * block)

    def parts_of(piece):
        return SPLIT[piece]

    def hid_at(at, piece, source, part_of):
        index, first, wide = lanes_of(piece)
        if wide > block:
            wide = wide // parts_of(piece)
            return hid.at[at, index, pl.ds(row_shift(source), share), pl.ds(first + part_of * wide, wide)]
        rows = share // parts_of(piece)
        start = pl.multiple_of(row_shift(source) + part_of * rows, 16)
        return hid.at[at, index, pl.ds(start, rows), pl.ds(first, wide)]

    def hid_sems(piece, hop, way, part_of):
        return hid_send, hid_recv.at[number(hid_keys, way, hop, piece, part_of)], ways[way]

    def hid_copy(piece, hop, way, part_of):
        source = (place + (n - hop + 1 if way == 0 else hop - 1)) % n
        return remote(hid_at(slot(hop - 1, way), piece, source, part_of), hid_at(slot(hop, way), piece, source, part_of),
                      *hid_sems(piece, hop, way, part_of))

    def hid_wait(piece, hop, way, part_of):
        source = (place + (n - hop if way == 0 else hop)) % n
        at = hid_at(slot(hop, way), piece, source, part_of)
        remote(at, at, *hid_sems(piece, hop, way, part_of)).wait_recv()

    def hid_rounds(piece, hop):
        return (piece % 2,) if hop == half else (0, 1)

    def swap(group, kind, wide):
        return remote(part.at[group, kind, :, pl.ds(0, wide)], theirs.at[group, kind, :, pl.ds(0, wide)],
                      part_send, part_recv.at[group], partner)

    def gate_up(group):
        slots = [0] if group == 0 else [1] if group == half else [2 * group, 2 * group + 1]
        wide = block * len(slots)
        if group == 0:
            loads[1].wait()
            loads[2].wait()
        else:
            for unit in range(UNITS - RING[group - 1]):
                for way in rounds(group, unit):
                    with jax.named_scope(f"ywait#g={group}#u={unit}#w={way}"):
                        y_copy(slot(group, way), unit, 1 - col).wait_recv()
        for kind in (0, 1):
            part[group, kind, :, :wide] = product(kind, 1 - core, slots)
            swap(group, kind, wide).start()
        for kind in (0, 1):
            keep[kind, :, :wide] = product(kind, core, slots)
        if group == 0:
            loads[3].wait()
            for copy in give:
                copy.start()
        with jax.named_scope(f"swapwait#g={group}"):
            both = theirs.at[group, :, :, pl.ds(0, wide)]
            remote(both, both, part_send, part_recv.at[group], partner).wait_recv()
        gate = keep[0, :, :wide] + theirs[group, 0, :, :wide]
        up = keep[1, :, :wide] + theirs[group, 1, :, :wide]
        index, first, wide = lanes_of(group)
        hid[0, index, pl.ds(row_shift(place), share), first:first + wide] = (
            gate / (1.0 + jnp.exp(-gate)) * up).astype(BF16)
        for part_of in range(parts_of(group)):
            for way in (0, 1):
                hid_copy(group, 1, way, part_of).start()

    def token_hop(hop, unit):
        for way in rounds(hop, unit):
            with jax.named_scope(f"tokwait#h={hop}#u={unit}#w={way}"):
                tok_copy(hop, way, unit).wait_recv()
            if hop < half and unit < RING[hop] and way in rounds(hop + 1, unit):
                tok_copy(hop + 1, way, unit).start()
            if unit < UNITS - RING[hop - 1]:
                y_copy(slot(hop, way), unit, col).start()

    def hid_hop(piece, hop, part_of):
        for way in hid_rounds(piece, hop):
            with jax.named_scope(f"hidwait#p={piece}#h={hop}#q={part_of}#w={way}"):
                hid_wait(piece, hop, way, part_of)
            if hop < half and way in hid_rounds(piece, hop + 1):
                hid_copy(piece, hop + 1, way, part_of).start()

    def add_one(at, source, piece):
        index, first, wide = lanes_of(piece)
        at_row = row_at(source, n)
        same = 1 - (at_row // half - core) * (at_row // half - core)
        mine = (2 * (at_row % half) + core) * share // 128 * 128
        start = pl.multiple_of(same * mine + (1 - same) * (held + at_row % half * window), 128)
        term = lax.dot_general(down[:, pl.ds(start, window)], hid[at, index, :, first:first + wide],
                               (((1,), (0,)), ((), ())), preferred_element_type=F32)
        if piece in (0, half):
            total[(source + piece) % n] += term
        else:
            for k, token_block in enumerate(((source + n - piece) % n, (source + piece) % n)):
                total[token_block] += term[:, k * block:(k + 1) * block]

    def add_down(piece, hop):
        if not whole:
            whole.append(True)
            remote(given, given, down_send, down_recv, partner).wait_recv()
        if hop == 0:
            add_one(0, place, piece)
        elif hop == half:
            add_one(1, (place + half) % n, piece)
        else:
            @pl.loop(0, 2)
            def _(way):
                add_one(2 * hop + way, (place + n - hop + 2 * hop * way) % n, piece)

    to_col, to_core = z // 2, z % 2
    near_col = 1 - (col - to_col) * (col - to_col)
    near_core = 1 - (core - to_core) * (core - to_core)

    def handled(d, by):
        return (place + half) % n if d == half else (place + d + (n - 2 * d) * by) % n

    def keep_rows(which):
        return pl.ds(pl.multiple_of(which * middle, 16), middle)

    def sum_copy(d):
        return remote(total.at[handled(d, 1 - core)], other.at[d - 1], sum_send.at[d - 1], sum_recv.at[d - 1], partner)

    def col_copy(d):
        return remote(send_y.at[d - 1], from_y.at[d - 1], col_send.at[d - 1], col_recv.at[d - 1], beside)

    def out_copy(d):
        to = {"row": row_at(handled(d, core), n), "col": to_col, "depth": to_core}
        return remote(done.at[d - 1], land.at[x, col], out_send.at[d - 1], out_recv.at[x, col], to)

    def direct_copy():
        to = {"row": row_at(handled(1, core), n), "col": to_col, "depth": to_core}
        return remote(direct, land1.at[x, col], last_send.at[3], direct_recv.at[x, col], to)

    def near_copy():
        return remote(total.at[place], other0, last_send.at[0], last_recv.at[0], partner)

    def half_copy():
        return remote(total.at[place, keep_rows(1 - core)], half0, last_send.at[1], last_recv.at[1], partner)

    def far_copy():
        return remote(send0, land0.at[core], last_send.at[2], last_recv.at[2 + core], {"col": to_col, "depth": to_core})

    def only(d, who):
        return pl.when(core == who) if d == half else (lambda f: f())

    def final_1(d):
        if d:
            @only(d, 1)
            def _():
                sum_copy(d).start()
            return

        @pl.when(near_col * (1 - near_core) == 1)
        def _():
            near_copy().start()

        @pl.when(near_col == 0)
        def _():
            half_copy().start()

    def final_2(d):
        if d:
            @only(d, 0)
            def _():
                with jax.named_scope(f"sumwait#d={d}"):
                    sum_copy(d).wait_recv()
                at = handled(d, core)
                if d == 1:
                    direct[...] = (total[at] + other[d - 1]).astype(BF16)
                    direct_copy().start()
                    return
                send_y[d - 1] = (total[at, keep_rows(1 - col)] + other[d - 1, keep_rows(1 - col)]).astype(BF16)
                col_copy(d).start()
                own_half[d - 1] = total[at, keep_rows(col)] + other[d - 1, keep_rows(col)]
            return

        @pl.when(near_col == 0)
        def _():
            half_copy().wait_recv()
            send0[...] = (total[place, keep_rows(core)] + half0[...]).astype(BF16)
            far_copy().start()

    def final_3(d):
        if d:
            @only(d, 0)
            def _():
                if d == 1:
                    return
                with jax.named_scope(f"colwait#d={d}"):
                    col_copy(d).wait_recv()
                done[d - 1] = (own_half[d - 1] + from_y[d - 1].astype(F32)).astype(BF16)
                out_copy(d).start()
            return

        @pl.when(near_col * near_core == 1)
        def _():
            with jax.named_scope("lastwait"):
                near_copy().wait_recv()
                for which in (0, 1):
                    remote(send0, land0.at[which], last_send.at[2], last_recv.at[2 + which], beside).wait_recv()
            for which in (0, 1):
                rows = slice(which * middle, (which + 1) * middle)
                value = total[place, rows] + other0[rows] + land0[which].astype(F32)
                out_ref[pl.ds(pl.multiple_of(x * features + which * middle, 16), middle)] = value.astype(BF16)

    total[...] = jnp.zeros_like(total)
    gap = window - share
    for at in range(n):
        hop, way = (0, 0) if at == 0 else (half, 0) if at == 1 else (at // 2, at % 2)
        shift = row_shift((place + (n - hop if way == 0 else hop)) % n)
        unit = share % 128
        for k in range(gap // unit):
            below = jnp.where(k * unit < shift, 0, share)
            rows = pl.ds(pl.multiple_of(k * unit + below, unit), unit)
            for index in range(half):
                hid[at, index, rows, :] = jnp.zeros((unit, 2 * block), BF16)

    act = {"G": gate_up, "T": token_hop, "H": hid_hop, "A": add_down, "F1": final_1, "F2": final_2, "F3": final_3}
    for name, *args in PLAN:
        with jax.named_scope(name + "_" + "_".join(map(str, args))):
            act[name](*args)

    with jax.named_scope("outwait"):
        for xx in (0, 1):
            from_z = half // 2 * col + core
            away = (place + n - (n - 1 - from_z if xx else from_z)) % n
            beside_me = 1 - jnp.minimum((away - 1) * (away - 1) * (away - n + 1) * (away - n + 1), 1)

            @pl.when((1 - beside_me) * away > 0)
            def _():
                for yy in (0, 1):
                    remote(land.at[xx, yy], land.at[xx, yy], out_send.at[0], out_recv.at[xx, yy], beside).wait_recv()
                    first = xx * features + yy * middle
                    out_ref[first:first + middle] = land[xx, yy]

            @pl.when(beside_me > 0)
            def _():
                for yy in (0, 1):
                    remote(direct, land1.at[xx, yy], last_send.at[3], direct_recv.at[xx, yy], beside).wait_recv()
                value = land1[xx, 0].astype(F32) + land1[xx, 1].astype(F32)
                out_ref[xx * features:(xx + 1) * features] = value.astype(BF16)
    with jax.named_scope("sendwait"):
        for d in range(1, half + 1):
            @only(d, 1)
            def _():
                sum_copy(d).wait_send()

            @only(d, 0)
            def _():
                if d == 1:
                    direct_copy().wait_send()
                    return
                col_copy(d).wait_send()
                out_copy(d).wait_send()

        @pl.when(near_col * (1 - near_core) == 1)
        def _():
            near_copy().wait_send()

        @pl.when(near_col == 0)
        def _():
            half_copy().wait_send()
            far_copy().wait_send()
        tok_sent, y_sent = (tok.at[box_of(k * unit_rows, n, block, tok.shape[2])] for k in counts[:2])
        hid_sent, part_sent = hid.at[0:n - 1, :, pl.ds(0, share)], part.at[0:half]
        for sent, sem in ((tok_sent, tok_send), (y_sent, y_send), (hid_sent, hid_send), (part_sent, part_send),
                          (given, down_send)):
            remote(sent, sent, sem, last_recv.at[0], partner).wait_send()


def fused_block(n, tokens, gate_weight, up_weight, down_weight):
    block, width = tokens.shape
    units = gate_weight.shape[0]
    held, features = down_weight.shape
    half, share = n // 2, units // 2
    window = (share + 127) // 128 * 128
    middle = features // 2
    counts = (2 * sum(RING[:-1]) + RING[-1], (n - 1) * UNITS - 2 * sum(RING[:-1]) - RING[-1],
              (n - 1) * sum(SPLIT))
    dma = pltpu.SemaphoreType.DMA
    result = pl.pallas_call(
        functools.partial(kernel, n, counts),
        out_shape=jax.ShapeDtypeStruct((2 * features, block), BF16),
        in_specs=[pl.BlockSpec(memory_space=pltpu.HBM)] * 4,
        out_specs=pl.BlockSpec(memory_space=pltpu.VMEM),
        scratch_shapes=[
            pltpu.VMEM((n, block, width), BF16),
            pltpu.VMEM((2, units, width), BF16),
            pltpu.VMEM((features, held + half * window), BF16),
            pltpu.VMEM((half + 1, 2, share, 2 * block), F32),
            pltpu.VMEM((2, share, 2 * block), F32),
            pltpu.VMEM((half + 1, 2, share, 2 * block), F32),
            pltpu.VMEM((n, half, window, 2 * block), BF16),
            pltpu.VMEM((n, features, block), F32),
            pltpu.VMEM((half, features, block), F32),
            pltpu.VMEM((half, middle, block), F32),
            pltpu.VMEM((half, middle, block), BF16),
            pltpu.VMEM((half, middle, block), BF16),
            pltpu.VMEM((half, middle, block), BF16),
            pltpu.VMEM((2, 2, middle, block), BF16),
            pltpu.VMEM((features, block), BF16),
            pltpu.VMEM((2, 2, features, block), BF16),
            pltpu.VMEM((features, block), F32),
            pltpu.VMEM((middle, block), F32),
            pltpu.VMEM((middle, block), BF16),
            pltpu.VMEM((2, middle, block), BF16),
            dma((4,)), dma(()), dma(()),
            dma(()), dma((counts[0],)),
            dma(()), dma((counts[1],)),
            dma(()), dma((half + 1,)),
            dma(()), dma((counts[2],)),
            dma((half,)), dma((half,)),
            dma((half,)), dma((half,)),
            dma((half,)), dma((2, 2)),
            dma((4,)), dma((4,)), dma((2, 2)),
        ],
        compiler_params=pltpu.CompilerParams(
            collective_id=0, has_side_effects=True, vmem_limit_bytes=54528 * 1024
        ),
    )(tokens, gate_weight, up_weight, down_weight.T)
    return result.T


def send_out(mine, rows, cols, depths):
    quarters = cols * depths
    per = rows // quarters
    block = mine.shape[0] // per
    width = mine.shape[1]
    row = lax.axis_index("row")
    low = row % per
    got = jnp.zeros((block, per, width), jnp.bfloat16)
    for k in range(per):
        pairs = []
        for r in range(rows):
            for q in range(quarters):
                a, e = r // per, r % per
                to_row = q * per + (e + k) % per
                pairs.append((r * quarters + q, to_row * quarters + a))
        piece = lax.dynamic_slice_in_dim(mine, (low + k) % per * block, block, 0)
        piece = lax.ppermute(piece, ("row", "col", "depth"), pairs)
        got = lax.dynamic_update_slice_in_dim(got, piece[:, None], (low - k) % per, 1)
    return got.reshape(block, per * width)


def solution(mesh):
    rows, cols, depths = (mesh.shape[a] for a in ("row", "col", "depth"))

    def local(tokens, gate_weight, up_weight, down_weight):
        units = gate_weight.shape[0]
        every = lax.all_gather(tokens, "row", axis=0, tiled=True)
        down = down_weight.reshape(rows // depths, depths, units // depths, -1)
        down = lax.all_to_all(down, "depth", split_axis=1, concat_axis=0, tiled=True)
        down = down.reshape(rows, units // depths, -1)
        paired = jnp.stack([gate_weight, up_weight])
        sums = jnp.einsum("td,gfd->gtf", every, paired, preferred_element_type=jnp.float32)
        sums = lax.psum_scatter(sums, "depth", scatter_dimension=2, tiled=True)
        hidden = (jax.nn.silu(sums[0]) * sums[1]).astype(jnp.bfloat16)
        hidden = lax.all_gather(hidden, "row", axis=0)
        partial = jnp.einsum("rtk,rkc->tc", hidden, down, preferred_element_type=jnp.float32)
        mine = lax.psum_scatter(partial, ("col", "depth"), scatter_dimension=0, tiled=True)
        return send_out(mine.astype(BF16), rows, cols, depths)

    def fused(*args):
        return fused_block(rows, *args)

    in_specs = (
        P("row", "depth"),
        P(("col", "row"), "depth"),
        P(("col", "row"), "depth"),
        P(("col", "depth"), "row"),
    )
    out_specs = P("row", ("col", "depth"))
    small = cols == 2 and depths == 2 and rows == 8
    return jax.shard_map(fused if small else local, mesh=mesh, in_specs=in_specs, out_specs=out_specs, check_vma=False)
```

```python
import functools

import jax
import jax.numpy as jnp
from jax import lax
from jax.experimental import pallas as pl
from jax.experimental.pallas import tpu as pltpu
from jax.sharding import PartitionSpec as P

MESH = pl.DeviceIdType.MESH
F32 = jnp.float32
BF16 = jnp.bfloat16


def row_at(place, n):
    back = place // (n // 2)
    return 2 * place * (1 - back) + (2 * (n - 1 - place) + 1) * back


UNITS, DIRECT = 8, 1
SPLIT = (1, 2, 2, 2, 2)
RING = (5, 4, 4, 4)
PLAN = [
    ("T", 1, 0), ("T", 1, 1), ("T", 1, 2), ("T", 2, 0), ("T", 2, 1), ("T", 1, 3), ("G", 0), ("T", 2, 2),
    ("T", 1, 4), ("G", 1), ("T", 2, 3), ("T", 3, 0), ("H", 1, 1, 0), ("H", 0, 1, 0), ("T", 3, 1), ("T", 3, 2),
    ("H", 1, 1, 1), ("T", 3, 3), ("G", 2), ("H", 0, 2, 0), ("T", 4, 0), ("H", 1, 2, 0), ("H", 2, 1, 1), ("T", 4, 1),
    ("T", 4, 2), ("H", 1, 2, 1), ("T", 4, 3), ("A", 0, 1), ("H", 2, 1, 0), ("H", 0, 3, 0), ("H", 2, 2, 1),
    ("H", 1, 3, 0), ("G", 3), ("A", 1, 1), ("H", 1, 3, 1), ("A", 0, 0), ("H", 2, 3, 1), ("H", 2, 2, 0), ("A", 2, 2),
    ("H", 3, 1, 0), ("G", 4), ("H", 3, 1, 1), ("A", 0, 3), ("H", 1, 4, 0), ("A", 1, 2), ("A", 0, 2), ("A", 2, 1),
    ("H", 3, 2, 0), ("H", 0, 4, 0), ("A", 1, 0), ("A", 1, 3), ("H", 4, 1, 1), ("H", 1, 4, 1), ("A", 3, 0),
    ("H", 4, 1, 0), ("A", 1, 4), ("A", 4, 1), ("H", 2, 4, 1), ("H", 3, 2, 1), ("H", 2, 3, 0), ("A", 2, 3),
    ("A", 3, 1), ("H", 3, 3, 0), ("A", 3, 2), ("A", 2, 0), ("H", 4, 2, 1), ("F1", 3), ("A", 4, 0), ("H", 4, 2, 0),
    ("A", 0, 4), ("F1", 4), ("A", 4, 2), ("F2", 3), ("H", 3, 3, 1), ("A", 3, 3), ("H", 3, 4, 0), ("H", 2, 4, 0),
    ("F2", 4), ("A", 2, 4), ("F1", 2), ("H", 4, 3, 1), ("H", 4, 3, 0), ("F2", 2), ("A", 4, 3), ("H", 3, 4, 1),
    ("F3", 3), ("A", 3, 4), ("F1", 1), ("H", 4, 4, 1), ("F2", 1), ("H", 4, 4, 0), ("F3", 4), ("A", 4, 4), ("F3", 2),
    ("F1", 0), ("F2", 0), ("F3", 0),
]


def box_of(rows, n, block, width):
    total = rows * width
    for k in range(n, 0, -1):
        for r in range(block, 0, -16):
            wide = total // (k * r)
            if k * r * wide == total and wide % 128 == 0 and wide <= width:
                return slice(0, k), pl.ds(0, r), pl.ds(0, wide)


def kernel(n, counts, tok_hbm, gate_hbm, up_hbm, down_hbm, out_ref, tok, weights, down, part, keep, theirs, hid, total, other,
           own_half, send_y, from_y, done, land, direct, land1, other0, half0, send0, land0, load_sem, down_send, down_recv,
           tok_send, tok_recv, y_send, y_recv, part_send, part_recv, hid_send, hid_recv, sum_send, sum_recv,
           col_send, col_recv, out_send, out_recv, last_send, last_recv, direct_recv):
    row, col, core = lax.axis_index("row"), lax.axis_index("col"), lax.axis_index("depth")
    half = n // 2
    x, z = row % 2, row // 2
    place = z * (1 - x) + (n - 1 - z) * x
    ways = ({"row": row_at((place + 1) % n, n)}, {"row": row_at((place + n - 1) % n, n)})
    beside, partner = {"col": 1 - col}, {"depth": 1 - core}
    block = tok_hbm.shape[0]
    units = gate_hbm.shape[0]
    share = units // 2
    features, held = down_hbm.shape
    middle = features // 2
    window = hid.shape[2]
    unit_rows = block // UNITS

    def remote(src, dst, send, recv, to):
        return pltpu.make_async_remote_copy(src_ref=src, dst_ref=dst, send_sem=send, recv_sem=recv,
                                            device_id=to, device_id_type=MESH)

    loads = [pltpu.make_async_copy(tok_hbm, tok.at[0], load_sem.at[0]),
             pltpu.make_async_copy(gate_hbm, weights.at[0], load_sem.at[1]),
             pltpu.make_async_copy(up_hbm, weights.at[1], load_sem.at[2]),
             pltpu.make_async_copy(down_hbm, down.at[:, pl.ds(0, held)], load_sem.at[3])]
    for copy in loads[:3]:
        copy.start()
    barrier = pltpu.get_barrier_semaphore()
    for peer in ways + (beside, partner):
        pl.semaphore_signal(barrier, inc=1, device_id=peer, device_id_type=MESH)
    with jax.named_scope("barrier"):
        pl.semaphore_wait(barrier, 4)
    with jax.named_scope("tokload"):
        loads[0].wait()

    def slot(hop, way):
        return 0 if hop == 0 else 1 if hop == half else 2 * hop + way

    def rounds(hop, unit):
        return (2 * unit // RING[hop - 1],) if hop == half else (0, 1)

    tok_keys, y_keys, hid_keys, whole = {}, {}, {}, []

    def number(keys, *key):
        return keys.setdefault(key, len(keys))

    def unit_at(unit, side):
        return pl.ds(pl.multiple_of(unit_rows * (unit * (1 - side) + (UNITS - 1 - unit) * side), unit_rows), unit_rows)

    across = [1 - jnp.minimum((place % half - half // 2 + 1 - way) * (place % half - half // 2 + 1 - way), 1)
              for way in (0, 1)]
    last_way = [{"row": across[way] * (row + 1 - 2 * x) + (1 - across[way]) * ways[way]["row"]} for way in (0, 1)]

    def via(hop, way):
        if hop < half:
            return slot(hop - 1, way), ways[way]
        return across[way] * slot(1, 1 - way) + (1 - across[way]) * slot(half - 1, way), last_way[way]

    def tok_copy(hop, way, unit):
        rows = unit_at(unit, col)
        source, to = via(hop, way)
        return remote(tok.at[source, rows], tok.at[slot(hop, way), rows],
                      tok_send, tok_recv.at[number(tok_keys, way, hop, unit)], to)

    def y_copy(at, unit, side):
        rows = unit_at(unit, side)
        return remote(tok.at[at, rows], tok.at[at, rows], y_send, y_recv.at[number(y_keys, at, unit)], beside)

    for unit in range(RING[0]):
        for way in (0, 1):
            tok_copy(1, way, unit).start()
    loads[3].start()

    def row_shift(source):
        return pl.multiple_of(source // half * 2 * (share % 128) + core * (share % 128), share % 128)

    given = down.at[:, pl.ds(held, half * window)]
    give = []
    for i in range(half):
        q = 2 * i + 1 - core
        lanes = pl.ds(pl.multiple_of(q * share // 128 * 128, 128), window)
        give.append(remote(down.at[:, lanes], down.at[:, pl.ds(held + i * window, window)],
                           down_send, down_recv, partner))

    def product(kind, which, slots):
        rows = pl.ds(pl.multiple_of(which * share, 16), share)
        seen = tok[slots[0]:slots[0] + len(slots)].reshape(block * len(slots), tok.shape[2])
        return lax.dot_general(weights[kind, rows, :], seen, (((1,), (1,)), ((), ())), preferred_element_type=F32)

    def lanes_of(piece):
        return (half - 1, 0, block) if piece == 0 else (half - 1, block, block) if piece == half else (
            piece - 1, 0, 2 * block)

    def parts_of(piece):
        return SPLIT[piece]

    def hid_at(at, piece, source, part_of):
        index, first, wide = lanes_of(piece)
        if wide > block:
            wide = wide // parts_of(piece)
            return hid.at[at, index, pl.ds(row_shift(source), share), pl.ds(first + part_of * wide, wide)]
        rows = share // parts_of(piece)
        start = pl.multiple_of(row_shift(source) + part_of * rows, 16)
        return hid.at[at, index, pl.ds(start, rows), pl.ds(first, wide)]

    def hid_sems(piece, hop, way, part_of):
        return hid_send, hid_recv.at[number(hid_keys, way, hop, piece, part_of)], via(hop, way)[1]

    def hid_copy(piece, hop, way, part_of):
        source = (place + (n - hop + 1 if way == 0 else hop - 1)) % n
        if hop == half:
            source = (across[way] * (place + n + 1 - 2 * way) + (1 - across[way]) * source) % n
        held_at = via(hop, way)[0]
        return remote(hid_at(held_at, piece, source, part_of), hid_at(slot(hop, way), piece, source, part_of),
                      *hid_sems(piece, hop, way, part_of))

    def hid_wait(piece, hop, way, part_of):
        source = (place + (n - hop if way == 0 else hop)) % n
        at = hid_at(slot(hop, way), piece, source, part_of)
        remote(at, at, *hid_sems(piece, hop, way, part_of)).wait_recv()

    def hid_rounds(piece, hop):
        return (piece % 2,) if hop == half else (0, 1)

    def swap(group, kind, wide):
        return remote(part.at[group, kind, :, pl.ds(0, wide)], theirs.at[group, kind, :, pl.ds(0, wide)],
                      part_send, part_recv.at[group], partner)

    def gate_up(group):
        slots = [0] if group == 0 else [1] if group == half else [2 * group, 2 * group + 1]
        wide = block * len(slots)
        if group == 0:
            loads[1].wait()
            loads[2].wait()
        else:
            for unit in range(UNITS - RING[group - 1]):
                for way in rounds(group, unit):
                    with jax.named_scope(f"ywait#g={group}#u={unit}#w={way}"):
                        y_copy(slot(group, way), unit, 1 - col).wait_recv()
        for kind in (0, 1):
            part[group, kind, :, :wide] = product(kind, 1 - core, slots)
            swap(group, kind, wide).start()
        for kind in (0, 1):
            keep[kind, :, :wide] = product(kind, core, slots)
        if group == 0:
            loads[3].wait()
            for copy in give:
                copy.start()
        with jax.named_scope(f"swapwait#g={group}"):
            both = theirs.at[group, :, :, pl.ds(0, wide)]
            remote(both, both, part_send, part_recv.at[group], partner).wait_recv()
        gate = keep[0, :, :wide] + theirs[group, 0, :, :wide]
        up = keep[1, :, :wide] + theirs[group, 1, :, :wide]
        index, first, wide = lanes_of(group)
        hid[0, index, pl.ds(row_shift(place), share), first:first + wide] = (
            gate / (1.0 + jnp.exp(-gate)) * up).astype(BF16)
        for part_of in range(parts_of(group)):
            for way in (0, 1):
                hid_copy(group, 1, way, part_of).start()

    def token_hop(hop, unit):
        for way in rounds(hop, unit):
            with jax.named_scope(f"tokwait#h={hop}#u={unit}#w={way}"):
                tok_copy(hop, way, unit).wait_recv()
            if hop < half and unit < RING[hop] and way in rounds(hop + 1, unit):
                tok_copy(hop + 1, way, unit).start()
            if unit < UNITS - RING[hop - 1]:
                y_copy(slot(hop, way), unit, col).start()

    def hid_hop(piece, hop, part_of):
        for way in hid_rounds(piece, hop):
            with jax.named_scope(f"hidwait#p={piece}#h={hop}#q={part_of}#w={way}"):
                hid_wait(piece, hop, way, part_of)
            if hop < half and way in hid_rounds(piece, hop + 1):
                hid_copy(piece, hop + 1, way, part_of).start()

    def add_one(at, source, piece):
        index, first, wide = lanes_of(piece)
        at_row = row_at(source, n)
        same = 1 - (at_row // half - core) * (at_row // half - core)
        mine = (2 * (at_row % half) + core) * share // 128 * 128
        start = pl.multiple_of(same * mine + (1 - same) * (held + at_row % half * window), 128)
        term = lax.dot_general(down[:, pl.ds(start, window)], hid[at, index, :, first:first + wide],
                               (((1,), (0,)), ((), ())), preferred_element_type=F32)
        if piece in (0, half):
            total[(source + piece) % n] += term
        else:
            for k, token_block in enumerate(((source + n - piece) % n, (source + piece) % n)):
                total[token_block] += term[:, k * block:(k + 1) * block]

    def add_down(piece, hop):
        if not whole:
            whole.append(True)
            remote(given, given, down_send, down_recv, partner).wait_recv()
        if hop == 0:
            add_one(0, place, piece)
        elif hop == half:
            add_one(1, (place + half) % n, piece)
        else:
            @pl.loop(0, 2)
            def _(way):
                add_one(2 * hop + way, (place + n - hop + 2 * hop * way) % n, piece)

    to_col, to_core = z // 2, z % 2
    near_col = 1 - (col - to_col) * (col - to_col)
    near_core = 1 - (core - to_core) * (core - to_core)

    def handled(d, by):
        return (place + half) % n if d == half else (place + d + (n - 2 * d) * by) % n

    def keep_rows(which):
        return pl.ds(pl.multiple_of(which * middle, 16), middle)

    def sum_copy(d):
        return remote(total.at[handled(d, 1 - core)], other.at[d - 1], sum_send.at[d - 1], sum_recv.at[d - 1], partner)

    def col_copy(d):
        return remote(send_y.at[d - 1], from_y.at[d - 1], col_send.at[d - 1], col_recv.at[d - 1], beside)

    def out_copy(d):
        to = {"row": row_at(handled(d, core), n), "col": to_col, "depth": to_core}
        return remote(done.at[d - 1], land.at[x, col], out_send.at[d - 1], out_recv.at[x, col], to)

    def direct_copy(d):
        to = {"row": row_at(handled(d, core), n), "col": to_col, "depth": to_core}
        return remote(direct.at[d - 1], land1.at[x, col], last_send.at[2 + d], direct_recv.at[x, col], to)

    def near_copy():
        return remote(total.at[place], other0, last_send.at[0], last_recv.at[0], partner)

    def half_copy():
        return remote(total.at[place, keep_rows(1 - core)], half0, last_send.at[1], last_recv.at[1], partner)

    def far_copy():
        return remote(send0, land0.at[core], last_send.at[2], last_recv.at[2 + core], {"col": to_col, "depth": to_core})

    def only(d, who):
        return pl.when(core == who) if d == half else (lambda f: f())

    def final_1(d):
        if d:
            @only(d, 1)
            def _():
                sum_copy(d).start()
            return

        @pl.when(near_col * (1 - near_core) == 1)
        def _():
            near_copy().start()

        @pl.when(near_col == 0)
        def _():
            half_copy().start()

    def final_2(d):
        if d:
            @only(d, 0)
            def _():
                with jax.named_scope(f"sumwait#d={d}"):
                    sum_copy(d).wait_recv()
                at = handled(d, core)
                if d <= DIRECT:
                    direct[d - 1] = (total[at] + other[d - 1]).astype(BF16)
                    direct_copy(d).start()
                    return
                send_y[d - 1] = (total[at, keep_rows(1 - col)] + other[d - 1, keep_rows(1 - col)]).astype(BF16)
                col_copy(d).start()
                own_half[d - 1] = total[at, keep_rows(col)] + other[d - 1, keep_rows(col)]
            return

        @pl.when(near_col == 0)
        def _():
            half_copy().wait_recv()
            send0[...] = (total[place, keep_rows(core)] + half0[...]).astype(BF16)
            far_copy().start()

    def final_3(d):
        if d:
            @only(d, 0)
            def _():
                if d <= DIRECT:
                    return
                with jax.named_scope(f"colwait#d={d}"):
                    col_copy(d).wait_recv()
                done[d - 1] = (own_half[d - 1] + from_y[d - 1].astype(F32)).astype(BF16)
                out_copy(d).start()
            return

        @pl.when(near_col * near_core == 1)
        def _():
            with jax.named_scope("lastwait"):
                near_copy().wait_recv()
                for which in (0, 1):
                    remote(send0, land0.at[which], last_send.at[2], last_recv.at[2 + which], beside).wait_recv()
            for which in (0, 1):
                rows = slice(which * middle, (which + 1) * middle)
                value = total[place, rows] + other0[rows] + land0[which].astype(F32)
                out_ref[pl.ds(pl.multiple_of(x * features + which * middle, 16), middle)] = value.astype(BF16)

    total[...] = jnp.zeros_like(total)
    gap = window - share
    for at in range(n):
        hop, way = (0, 0) if at == 0 else (half, 0) if at == 1 else (at // 2, at % 2)
        shift = row_shift((place + (n - hop if way == 0 else hop)) % n)
        unit = share % 128
        for k in range(gap // unit):
            below = jnp.where(k * unit < shift, 0, share)
            rows = pl.ds(pl.multiple_of(k * unit + below, unit), unit)
            for index in range(half):
                hid[at, index, rows, :] = jnp.zeros((unit, 2 * block), BF16)

    act = {"G": gate_up, "T": token_hop, "H": hid_hop, "A": add_down, "F1": final_1, "F2": final_2, "F3": final_3}
    for name, *args in PLAN:
        with jax.named_scope(name + "_" + "_".join(map(str, args))):
            act[name](*args)

    with jax.named_scope("outwait"):
        for xx in (0, 1):
            from_z = half // 2 * col + core
            away = (place + n - (n - 1 - from_z if xx else from_z)) % n
            away = jnp.minimum(away, n - away)

            @pl.when(away > DIRECT)
            def _():
                for yy in (0, 1):
                    remote(land.at[xx, yy], land.at[xx, yy], out_send.at[0], out_recv.at[xx, yy], beside).wait_recv()
                    first = xx * features + yy * middle
                    out_ref[first:first + middle] = land[xx, yy]

            @pl.when(away * (DIRECT + 1 - away) > 0)
            def _():
                for yy in (0, 1):
                    remote(direct.at[0], land1.at[xx, yy], last_send.at[3], direct_recv.at[xx, yy], beside).wait_recv()
                value = land1[xx, 0].astype(F32) + land1[xx, 1].astype(F32)
                out_ref[xx * features:(xx + 1) * features] = value.astype(BF16)
    with jax.named_scope("sendwait"):
        for d in range(1, half + 1):
            @only(d, 1)
            def _():
                sum_copy(d).wait_send()

            @only(d, 0)
            def _():
                if d <= DIRECT:
                    direct_copy(d).wait_send()
                    return
                col_copy(d).wait_send()
                out_copy(d).wait_send()

        @pl.when(near_col * (1 - near_core) == 1)
        def _():
            near_copy().wait_send()

        @pl.when(near_col == 0)
        def _():
            half_copy().wait_send()
            far_copy().wait_send()
        tok_sent, y_sent = (tok.at[box_of(k * unit_rows, n, block, tok.shape[2])] for k in counts[:2])
        hid_sent, part_sent = hid.at[0:n - 1, :, pl.ds(0, share)], part.at[0:half]
        for sent, sem in ((tok_sent, tok_send), (y_sent, y_send), (hid_sent, hid_send), (part_sent, part_send),
                          (given, down_send)):
            remote(sent, sent, sem, last_recv.at[0], partner).wait_send()


def fused_block(n, tokens, gate_weight, up_weight, down_weight):
    block, width = tokens.shape
    units = gate_weight.shape[0]
    held, features = down_weight.shape
    half, share = n // 2, units // 2
    window = (share + 127) // 128 * 128
    middle = features // 2
    counts = (2 * sum(RING[:-1]) + RING[-1], (n - 1) * UNITS - 2 * sum(RING[:-1]) - RING[-1],
              (n - 1) * sum(SPLIT))
    dma = pltpu.SemaphoreType.DMA
    result = pl.pallas_call(
        functools.partial(kernel, n, counts),
        out_shape=jax.ShapeDtypeStruct((2 * features, block), BF16),
        in_specs=[pl.BlockSpec(memory_space=pltpu.HBM)] * 4,
        out_specs=pl.BlockSpec(memory_space=pltpu.VMEM),
        scratch_shapes=[
            pltpu.VMEM((n, block, width), BF16),
            pltpu.VMEM((2, units, width), BF16),
            pltpu.VMEM((features, held + half * window), BF16),
            pltpu.VMEM((half + 1, 2, share, 2 * block), F32),
            pltpu.VMEM((2, share, 2 * block), F32),
            pltpu.VMEM((half + 1, 2, share, 2 * block), F32),
            pltpu.VMEM((n, half, window, 2 * block), BF16),
            pltpu.VMEM((n, features, block), F32),
            pltpu.VMEM((half, features, block), F32),
            pltpu.VMEM((half, middle, block), F32),
            pltpu.VMEM((half, middle, block), BF16),
            pltpu.VMEM((half, middle, block), BF16),
            pltpu.VMEM((half, middle, block), BF16),
            pltpu.VMEM((2, 2, middle, block), BF16),
            pltpu.VMEM((DIRECT, features, block), BF16),
            pltpu.VMEM((2, 2, features, block), BF16),
            pltpu.VMEM((features, block), F32),
            pltpu.VMEM((middle, block), F32),
            pltpu.VMEM((middle, block), BF16),
            pltpu.VMEM((2, middle, block), BF16),
            dma((4,)), dma(()), dma(()),
            dma(()), dma((counts[0],)),
            dma(()), dma((counts[1],)),
            dma(()), dma((half + 1,)),
            dma(()), dma((counts[2],)),
            dma((half,)), dma((half,)),
            dma((half,)), dma((half,)),
            dma((half,)), dma((2, 2)),
            dma((3 + DIRECT,)), dma((4,)), dma((2, 2)),
        ],
        compiler_params=pltpu.CompilerParams(
            collective_id=0, has_side_effects=True, vmem_limit_bytes=54528 * 1024
        ),
    )(tokens, gate_weight, up_weight, down_weight.T)
    return result.T


def send_out(mine, rows, cols, depths):
    quarters = cols * depths
    per = rows // quarters
    block = mine.shape[0] // per
    width = mine.shape[1]
    row = lax.axis_index("row")
    low = row % per
    got = jnp.zeros((block, per, width), jnp.bfloat16)
    for k in range(per):
        pairs = []
        for r in range(rows):
            for q in range(quarters):
                a, e = r // per, r % per
                to_row = q * per + (e + k) % per
                pairs.append((r * quarters + q, to_row * quarters + a))
        piece = lax.dynamic_slice_in_dim(mine, (low + k) % per * block, block, 0)
        piece = lax.ppermute(piece, ("row", "col", "depth"), pairs)
        got = lax.dynamic_update_slice_in_dim(got, piece[:, None], (low - k) % per, 1)
    return got.reshape(block, per * width)


def solution(mesh):
    rows, cols, depths = (mesh.shape[a] for a in ("row", "col", "depth"))

    def local(tokens, gate_weight, up_weight, down_weight):
        units = gate_weight.shape[0]
        every = lax.all_gather(tokens, "row", axis=0, tiled=True)
        down = down_weight.reshape(rows // depths, depths, units // depths, -1)
        down = lax.all_to_all(down, "depth", split_axis=1, concat_axis=0, tiled=True)
        down = down.reshape(rows, units // depths, -1)
        paired = jnp.stack([gate_weight, up_weight])
        sums = jnp.einsum("td,gfd->gtf", every, paired, preferred_element_type=jnp.float32)
        sums = lax.psum_scatter(sums, "depth", scatter_dimension=2, tiled=True)
        hidden = (jax.nn.silu(sums[0]) * sums[1]).astype(jnp.bfloat16)
        hidden = lax.all_gather(hidden, "row", axis=0)
        partial = jnp.einsum("rtk,rkc->tc", hidden, down, preferred_element_type=jnp.float32)
        mine = lax.psum_scatter(partial, ("col", "depth"), scatter_dimension=0, tiled=True)
        return send_out(mine.astype(BF16), rows, cols, depths)

    def fused(*args):
        return fused_block(rows, *args)

    in_specs = (
        P("row", "depth"),
        P(("col", "row"), "depth"),
        P(("col", "row"), "depth"),
        P(("col", "depth"), "row"),
    )
    out_specs = P("row", ("col", "depth"))
    small = cols == 2 and depths == 2 and rows == 8
    return jax.shard_map(fused if small else local, mesh=mesh, in_specs=in_specs, out_specs=out_specs, check_vma=False)
```
